32 devices in a mesh: groups: 2 (over x), blk: 16 (over z, y, core).
Axes of the slice: x: 2, y: 2, z: 4, core: 2. Of those that a mesh axis runs over, the one named last changes fastest.
Arguments:
- coords: float32 [32, 24576], P(None, ('groups', 'blk')), parts along dimension 1, may hold values from -6 to 6
- alpha: float32 [24576], P(('groups', 'blk')), parts along dimension 0, may hold values from -6 to 6
- probe_solves: float32 [15, 24576], P(None, ('groups', 'blk')), parts along dimension 1, may hold values from -6 to 6
- probes: float32 [15, 24576], P(None, ('groups', 'blk')), parts along dimension 1, may hold values from -6 to 6
- lengthscale: float32 [32], replicated, may hold values from 4 to 12
Outputs:
- grad: float32 [32, 24576], P(None, ('groups', 'blk')), parts along dimension 1
The draws below stay inside these ranges and needn't reach their ends.
There are 2 independent parts, one for each index of `groups`. The reference program is written for one: setup_inputs(seed, part) draws one part's arguments, and reference() takes and returns one part's arrays. A program takes and returns all parts, laid end to end along the dimension named above; an argument that names none is the same for every part. Nothing has to cross between parts.
All inputs are finite; a program needn't handle non-finite values.
Results may differ from the reference program's by a relative error of at most 0.00014.
Values sent between devices are 32-bit elements; how exact they have to be, the bound alone decides.
A program may use at most 64 MiB of HBM per device.

```python
import math
import jax
import jax.numpy as jnp
from jax import lax

DIM = 32
PROBES = 15
BLOCK = 768
STEPS = 4
NPTS = 12288
N_BLK = 16


def levels(own_key, extent, shards, least, largest):
    level, own = 1.0, jax.random.fold_in(own_key, 6)
    for dim, blocks in shards:
        heights = jnp.exp(jax.random.uniform(jax.random.fold_in(own, dim), (blocks,), jnp.float32, least / len(shards), largest / len(shards)))
        level = level * jnp.repeat(heights, extent[dim] // blocks).reshape([-1 if axis == dim else 1 for axis in range(len(extent))])
    return level


def scatter_about(key, dims, deviation, most, split=(), dtype=jnp.bfloat16):
    drawn = deviation * jax.random.normal(key, dims, jnp.float32)
    if split:
        drawn = drawn * levels(key, dims, split, -0.22, 0.18)
    return jnp.clip(drawn, -most, most).astype(dtype)


def setup_inputs(seed: int = 0, part: int = 0) -> dict:
    seeds = jax.random.split(jax.random.key(seed), 6)
    part_splits = jax.random.split(jax.random.fold_in(seeds[5], part), 6)
    return {
        "coords": scatter_about(part_splits[0], (DIM, NPTS), 1.0, 6.0, ((1, 16),), jnp.float32),
        "alpha": scatter_about(part_splits[1], (NPTS,), 1.0, 6.0, ((0, 16),), jnp.float32),
        "probe_solves": scatter_about(part_splits[2], (PROBES, NPTS), 1.0, 6.0, ((1, 16),), jnp.float32),
        "probes": scatter_about(part_splits[3], (PROBES, NPTS), 1.0, 6.0, ((1, 16),), jnp.float32),
        "lengthscale": jnp.clip(jnp.exp(jax.random.uniform(seeds[4], (DIM,), jnp.float32, math.log(4.0), math.log(12.0))), 4.0, 12.0),
    }


root_five = 5.0 ** 0.5

def tile_terms(own_scaled, own_table, vis_scaled, vis_table):
    probe_count = (own_table.shape[0] - 1) // 2
    half_inv = 1.0 / (2.0 * probe_count)
    left_rows = jnp.concatenate([own_table[:1], -half_inv * own_table[1:]], 0)
    right_rows = jnp.concatenate([vis_table[:1], vis_table[1 + probe_count:], vis_table[1:1 + probe_count]], 0)
    contract_first = (((0,), (0,)), ((), ()))
    inner = lax.dot_general(own_scaled, vis_scaled, contract_first, precision=lax.Precision.HIGHEST, preferred_element_type=jnp.float32)
    own_square = lax.optimization_barrier(jnp.sum(own_scaled * own_scaled, 0))
    vis_square = lax.optimization_barrier(jnp.sum(vis_scaled * vis_scaled, 0))
    distance = own_square[:, None] + vis_square[None, :] - 2.0 * inner
    radius = jnp.sqrt(jnp.maximum(distance, 0.0))
    profile = (1.0 + root_five * radius) * jnp.exp(-root_five * radius)
    coupling = lax.dot_general(left_rows, right_rows, contract_first, precision=lax.Precision.HIGHEST, preferred_element_type=jnp.float32)
    weighted = coupling * profile
    row_part = own_scaled * lax.optimization_barrier(jnp.sum(weighted, 1))[None, :] - lax.dot_general(vis_scaled, weighted, (((1,), (1,)), ((), ())), precision=lax.Precision.HIGHEST, preferred_element_type=jnp.float32)
    col_part = vis_scaled * lax.optimization_barrier(jnp.sum(weighted, 0))[None, :] - jnp.dot(own_scaled, weighted, precision=lax.Precision.HIGHEST, preferred_element_type=jnp.float32)
    return (row_part, col_part)

def reference(coords, alpha, probe_solves, probes, lengthscale):
    scaled = coords / lengthscale[:, None]
    table = jnp.concatenate([alpha[None], probe_solves, probes], 0)
    blocks_scaled = scaled.reshape(DIM, N_BLK, BLOCK).transpose(1, 0, 2)
    blocks_table = table.reshape(table.shape[0], N_BLK, BLOCK).transpose(1, 0, 2)
    row_total = jnp.zeros(blocks_scaled.shape, jnp.float32)
    col_total = jnp.zeros(blocks_scaled.shape, jnp.float32)
    for offset in range(1, STEPS + 1):
        vis_scaled = jnp.roll(blocks_scaled, -offset, axis=0)
        vis_table = jnp.roll(blocks_table, -offset, axis=0)
        rows_now, cols_now = lax.map(lambda pieces: tile_terms(pieces[0], pieces[1], pieces[2], pieces[3]), (blocks_scaled, blocks_table, vis_scaled, vis_table))
        row_total = row_total + rows_now
        col_total = col_total + jnp.roll(cols_now, offset, axis=0)
    summed = (row_total + col_total).transpose(1, 0, 2).reshape(DIM, N_BLK * BLOCK)
    return -(5.0 / 3.0) / lengthscale[:, None] * summed
```

```python
import functools
import math

import jax
import jax.numpy as jnp
from jax import lax
from jax.experimental import pallas as pl
from jax.experimental.pallas import tpu as pltpu
from jax.sharding import PartitionSpec as P

unit = 5.0**0.5 * math.log2(math.e)
ln_two = math.log(2.0)
inv_ln_two = 1.0 / ln_two
f32, bf16 = jnp.float32, jnp.bfloat16
row_chunk = 256
piece = 256


def pieces(x):
    high = x.astype(bf16)
    rest = x - high.astype(f32)
    mid = rest.astype(bf16)
    low = (rest - mid.astype(f32)).astype(bf16)
    return high, mid, low


def norm_rows(field, own):
    high, mid, low = (p.astype(f32) for p in pieces(jnp.sum(field * field, 0, keepdims=True)))
    row = lax.broadcasted_iota(jnp.int32, (16, field.shape[1]), 0)
    first = 0 if own else 3
    ones = (row >= 3 - first) & (row < 6 - first)
    out = jnp.where(ones, 1.0, 0.0)
    for at, piece in enumerate((high, mid, low)):
        out = jnp.where(row == first + at, piece, out)
    return out.astype(bf16)


def kernel(
    dims, steps, count, coords, alpha, solves, probes, lengths, out,
    msg, recv, left_d, left_c, right_d, right_c, acc, send_sem, recv_sem,
):
    me = lax.axis_index("blk")
    core = lax.rem(me, 2)
    side = lax.rem(me // 2, 2)
    partner = {"blk": me + 1 - 2 * core}
    mate = {"blk": me + 2 - 4 * side}
    rows, block = msg.shape
    width = (rows - dims) // 2
    msg[:dims, :] = coords[...]
    msg[dims : dims + width, :] = jnp.concatenate([solves[...], alpha[...]], 0)
    msg[dims + width :, :] = jnp.concatenate([probes[...], jnp.zeros_like(alpha)], 0)

    def at(offset):
        return {"blk": lax.rem(me + offset + count, count)}

    offsets = [sign * k for k in range(4, steps + 1, 4) for sign in (1, -1)]
    straight = {k: i for i, k in enumerate(offsets)}
    straights = len(offsets)
    rails = 2 * straights
    barrier = pltpu.get_barrier_semaphore()
    devices = [at(k) for k in offsets] + [mate, partner]
    for device in devices:
        pl.semaphore_signal(barrier, inc=1, device_id=device, device_id_type=pl.DeviceIdType.MESH)
    pl.semaphore_wait(barrier, len(devices))

    copies = {}
    parts = block // piece

    def send(src, slot, part, device):
        columns = pl.ds(part * piece, piece)
        copy = pltpu.make_async_remote_copy(
            src_ref=src.at[:, columns],
            dst_ref=recv.at[slot, :, columns],
            send_sem=send_sem.at[slot, part],
            recv_sem=recv_sem.at[slot, part],
            device_id=device,
            device_id_type=pl.DeviceIdType.MESH,
        )
        copy.start()
        copies[slot, part] = copy

    def arrive(slot, part):
        copies[slot, part].wait_recv()

    for part in range(parts):
        send(msg, rails, part, partner)
        for k in offsets:
            send(msg, straight[-k], part, at(k))
        send(msg, straights, part, mate)

    dim = lax.broadcasted_iota(jnp.int32, (dims, 128), 0)
    length = jnp.full((dims, 128), 1.0, f32)
    for d in range(dims):
        length = jnp.where(dim == d, lengths[d], length)
    length = length[:, :1]
    inverse = unit / length

    field = msg[:dims, :] * inverse
    high, mid, low = pieces(-2.0 * field)
    left_d[...] = jnp.concatenate([high, high, high, norm_rows(field, True), mid, mid, low], 0).T
    row = lax.broadcasted_iota(jnp.int32, (width, block), 0)
    scale = -ln_two / (2.0 * (width - 1))
    top, bottom = msg[dims : dims + width, :], msg[dims + width :, :]
    first = jnp.where(row == width - 1, ln_two * top, scale * bottom)
    second = jnp.where(row == width - 1, 0.0, scale * top)
    high, mid, low = pieces(jnp.concatenate([first, second], 0))
    left_c[...] = jnp.concatenate([high, high, high, mid, mid, low], 0).T

    done = [0]

    def visit(slot, part):
        buffer, fresh = done[0] % 2, done[0] == 0
        done[0] += 1
        columns = pl.ds(part * piece, piece)
        field = recv[slot, :dims, columns] * inverse
        high, mid, low = pieces(field)
        right_d[buffer] = jnp.concatenate([high, mid, low, norm_rows(field, False), high, mid, high], 0)
        table = recv[slot, dims:, columns]
        high, mid, low = pieces(table)
        right_c[buffer] = jnp.concatenate([high, mid, low, high, mid, high], 0)
        across = right_d[buffer, : 3 * dims + 16, :]
        for start in range(0, block, row_chunk):
            lines = pl.ds(start, row_chunk)
            distance = jnp.dot(left_d[lines, :], right_d[buffer], preferred_element_type=f32)
            coupling = jnp.dot(left_c[lines, :], right_c[buffer], preferred_element_type=f32)
            distance = jnp.maximum(distance, 1e-30)
            radius = distance * lax.rsqrt(distance)
            weighted = coupling * ((radius + inv_ln_two) * jnp.exp2(-radius))
            w_high = weighted.astype(bf16)
            w_low = (weighted - w_high.astype(f32)).astype(bf16)
            contract = (((1,), (1,)), ((), ()))
            part_sum = lax.dot_general(w_high, across, contract, preferred_element_type=f32)
            part_sum += lax.dot_general(w_low, across, contract, preferred_element_type=f32)
            if fresh and part == 0:
                acc[lines, :] = part_sum
            else:
                acc[lines, :] += part_sum

    every = range(parts)
    for part in every:
        arrive(rails, part)
        visit(rails, part)

    mated, crossed = straights, rails
    for k in range(4, steps + 1, 4):
        plus, minus = straight[k], straight[-k]
        last = k == steps
        for part in every:
            if k == 4:
                arrive(straights, part)
                send(recv.at[straights], rails + 1, part, partner)
                visit(straights, part)
            arrive(plus, part)
            arrive(minus, part)
            if last:
                send(recv.at[plus + side], straights + 1 + plus, part, mate)
                send(recv.at[plus + core], rails + 2 + plus, part, partner)
            else:
                for slot in (plus, minus):
                    send(recv.at[slot], straights + 1 + slot, part, mate)
                    send(recv.at[slot], rails + 2 + slot, part, partner)
            if k == 4:
                arrive(rails + 1, part)
                visit(rails + 1, part)
            visit(plus, part)
            visit(minus, part)
    ends = rails + 1 + straights
    for slot in range(straights + 1, rails):
        for part in every:
            arrive(slot, part)
            send(recv.at[slot], ends + slot - straights - 1, part, partner)
            arrive(rails + 1 + slot - straights, part)
            visit(rails + 1 + slot - straights, part)
            visit(slot, part)
    for slot in range(ends, 2 * rails):
        for part in every:
            arrive(slot, part)
            visit(slot, part)
    total = acc[...].T
    moved = total[:dims] + total[dims : 2 * dims] + total[2 * dims : 3 * dims]
    field = msg[:dims, :] * inverse
    out[...] = (-(5.0 / 3.0) / unit / length) * (field * total[3 * dims : 3 * dims + 1] - moved)
    for copy in copies.values():
        copy.wait_send()


def on_device(coords, alpha, probe_solves, probes, lengthscale):
    count = lax.axis_size("blk")
    steps = count // 4
    dims, block = coords.shape
    table_rows = 2 * (probes.shape[0] + 1)
    rows = dims + table_rows
    depth_d, depth_c = 6 * dims + 16, 6 * table_rows
    parts = block // piece
    return pl.pallas_call(
        functools.partial(kernel, dims, steps, count),
        out_shape=jax.ShapeDtypeStruct((dims, block), f32),
        in_specs=[pl.BlockSpec(memory_space=pltpu.VMEM)] * 4 + [pl.BlockSpec(memory_space=pltpu.SMEM)],
        out_specs=pl.BlockSpec(memory_space=pltpu.VMEM),
        scratch_shapes=[
            pltpu.VMEM((rows, block), f32),
            pltpu.VMEM((2 * steps, rows, block), f32),
            pltpu.VMEM((block, depth_d), bf16),
            pltpu.VMEM((block, depth_c), bf16),
            pltpu.VMEM((2, depth_d, piece), bf16),
            pltpu.VMEM((2, depth_c, piece), bf16),
            pltpu.VMEM((block, 3 * dims + 16), f32),
            pltpu.SemaphoreType.DMA((2 * steps, parts)),
            pltpu.SemaphoreType.DMA((2 * steps, parts)),
        ],
        compiler_params=pltpu.CompilerParams(collective_id=0, has_side_effects=True),
    )(coords, alpha[None], probe_solves, probes, lengthscale)


def solution(mesh):
    return jax.shard_map(
        on_device,
        mesh=mesh,
        in_specs=(
            P(None, ("groups", "blk")),
            P(("groups", "blk")),
            P(None, ("groups", "blk")),
            P(None, ("groups", "blk")),
            P(),
        ),
        out_specs=P(None, ("groups", "blk")),
        check_vma=False,
    )
```

```python
import functools
import math

import jax
import jax.numpy as jnp
from jax import lax
from jax.experimental import pallas as pl
from jax.experimental.pallas import tpu as pltpu
from jax.sharding import PartitionSpec as P

unit = 5.0**0.5 * math.log2(math.e)
ln_two = math.log(2.0)
inv_ln_two = 1.0 / ln_two
f32, bf16 = jnp.float32, jnp.bfloat16
piece = 256


def pieces(x):
    high = x.astype(bf16)
    rest = x - high.astype(f32)
    mid = rest.astype(bf16)
    low = (rest - mid.astype(f32)).astype(bf16)
    return high, mid, low


def norm_rows(field, own):
    high, mid, low = (p.astype(f32) for p in pieces(jnp.sum(field * field, 0, keepdims=True)))
    row = lax.broadcasted_iota(jnp.int32, (16, field.shape[1]), 0)
    first = 0 if own else 3
    ones = (row >= 3 - first) & (row < 6 - first)
    out = jnp.where(ones, 1.0, 0.0)
    for at, piece in enumerate((high, mid, low)):
        out = jnp.where(row == first + at, piece, out)
    return out.astype(bf16)


def kernel(
    dims, steps, count, coords, alpha, solves, probes, lengths, out,
    msg, recv, left_d, left_c, right_d, right_c, acc, send_sem, recv_sem,
):
    me = lax.axis_index("blk")
    core = lax.rem(me, 2)
    side = lax.rem(me // 2, 2)
    partner = {"blk": me + 1 - 2 * core}
    mate = {"blk": me + 2 - 4 * side}
    rows, block = msg.shape
    width = (rows - dims) // 2
    msg[:dims, :] = coords[...]
    line = alpha[...].reshape(1, block)
    msg[dims : dims + width, :] = jnp.concatenate([solves[...], line], 0)
    msg[dims + width :, :] = jnp.concatenate([probes[...], jnp.zeros_like(line)], 0)

    def at(offset):
        return {"blk": lax.rem(me + offset + count, count)}

    offsets = [sign * k for k in range(4, steps + 1, 4) for sign in (1, -1)]
    straight = {k: i for i, k in enumerate(offsets)}
    straights = len(offsets)
    rails = 2 * straights
    barrier = pltpu.get_barrier_semaphore()
    devices = [at(k) for k in offsets] + [mate, partner]
    for device in devices:
        pl.semaphore_signal(barrier, inc=1, device_id=device, device_id_type=pl.DeviceIdType.MESH)
    pl.semaphore_wait(barrier, len(devices))

    copies = {}
    parts = block // piece

    def send(src, slot, part, device):
        columns = pl.ds(part * piece, piece)
        copy = pltpu.make_async_remote_copy(
            src_ref=src.at[:, columns],
            dst_ref=recv.at[slot, :, columns],
            send_sem=send_sem.at[slot, part],
            recv_sem=recv_sem.at[slot, part],
            device_id=device,
            device_id_type=pl.DeviceIdType.MESH,
        )
        copy.start()
        copies[slot, part] = copy

    def arrive(slot, part):
        copies[slot, part].wait_recv()

    for part in range(parts):
        send(msg, rails, part, partner)
        for k in offsets:
            send(msg, straight[-k], part, at(k))
        send(msg, straights, part, mate)

    dim = lax.broadcasted_iota(jnp.int32, (dims, 128), 0)
    length = jnp.full((dims, 128), 1.0, f32)
    for d in range(dims):
        length = jnp.where(dim == d, lengths[d], length)
    length = length[:, :1]
    inverse = unit / length

    field = msg[:dims, :] * inverse
    high, mid, low = pieces(-2.0 * field)
    left_d[...] = jnp.concatenate([high, high, high, norm_rows(field, True), mid, mid, low], 0).T
    row = lax.broadcasted_iota(jnp.int32, (width, block), 0)
    scale = -ln_two / (2.0 * (width - 1))
    top, bottom = msg[dims : dims + width, :], msg[dims + width :, :]
    first = jnp.where(row == width - 1, ln_two * top, scale * bottom)
    second = jnp.where(row == width - 1, 0.0, scale * top)
    high, mid, low = pieces(jnp.concatenate([first, second], 0))
    left_c[...] = jnp.concatenate([high, high, high, mid, mid, low], 0).T

    done = [0]

    def visit(slot, part):
        buffer, fresh = done[0] % 2, done[0] == 0
        done[0] += 1
        columns = pl.ds(part * piece, piece)
        field = recv[slot, :dims, columns] * inverse
        high, mid, low = pieces(field)
        right_d[buffer] = jnp.concatenate([high, mid, low, norm_rows(field, False), high, mid, high], 0)
        table = recv[slot, dims:, columns]
        high, mid, low = pieces(table)
        right_c[buffer] = jnp.concatenate([high, mid, low, high, mid, high], 0)
        across = right_d[buffer, : 3 * dims + 16, :]
        for start in (0,):
            lines = pl.ds(start, block)
            distance = jnp.dot(left_d[lines, :], right_d[buffer], preferred_element_type=f32)
            coupling = jnp.dot(left_c[lines, :], right_c[buffer], preferred_element_type=f32)
            distance = jnp.maximum(distance, 1e-30)
            radius = distance * lax.rsqrt(distance)
            weighted = coupling * ((radius + inv_ln_two) * jnp.exp2(-radius))
            w_high = weighted.astype(bf16)
            w_low = (weighted - w_high.astype(f32)).astype(bf16)
            contract = (((1,), (1,)), ((), ()))
            part_sum = lax.dot_general(w_high, across, contract, preferred_element_type=f32)
            part_sum += lax.dot_general(w_low, across, contract, preferred_element_type=f32)
            if fresh and part == 0:
                acc[lines, :] = part_sum
            else:
                acc[lines, :] += part_sum

    every = range(parts)
    for part in every:
        arrive(rails, part)
        visit(rails, part)

    mated, crossed = straights, rails
    for k in range(4, steps + 1, 4):
        plus, minus = straight[k], straight[-k]
        last = k == steps
        for part in every:
            if k == 4:
                arrive(straights, part)
                send(recv.at[straights], rails + 1, part, partner)
                visit(straights, part)
            arrive(plus, part)
            arrive(minus, part)
            if last:
                send(recv.at[plus + side], straights + 1 + plus, part, mate)
                send(recv.at[plus + core], rails + 2 + plus, part, partner)
            else:
                for slot in (plus, minus):
                    send(recv.at[slot], straights + 1 + slot, part, mate)
                    send(recv.at[slot], rails + 2 + slot, part, partner)
            if k == 4:
                arrive(rails + 1, part)
                visit(rails + 1, part)
            visit(plus, part)
            visit(minus, part)
    ends = rails + 1 + straights
    for slot in range(straights + 1, rails):
        for part in every:
            arrive(slot, part)
            send(recv.at[slot], ends + slot - straights - 1, part, partner)
            arrive(rails + 1 + slot - straights, part)
            visit(rails + 1 + slot - straights, part)
            visit(slot, part)
    for slot in range(ends, 2 * rails):
        for part in every:
            arrive(slot, part)
            visit(slot, part)
    total = acc[...].T
    moved = total[:dims] + total[dims : 2 * dims] + total[2 * dims : 3 * dims]
    field = msg[:dims, :] * inverse
    out[...] = (-(5.0 / 3.0) / unit / length) * (field * total[3 * dims : 3 * dims + 1] - moved)
    for copy in copies.values():
        copy.wait_send()


def on_device(coords, alpha, probe_solves, probes, lengthscale):
    count = lax.axis_size("blk")
    steps = count // 4
    dims, block = coords.shape
    table_rows = 2 * (probes.shape[0] + 1)
    rows = dims + table_rows
    depth_d, depth_c = 6 * dims + 16, 6 * table_rows
    parts = block // piece
    return pl.pallas_call(
        functools.partial(kernel, dims, steps, count),
        out_shape=jax.ShapeDtypeStruct((dims, block), f32),
        in_specs=[pl.BlockSpec(memory_space=pltpu.VMEM)] * 4 + [pl.BlockSpec(memory_space=pltpu.SMEM)],
        out_specs=pl.BlockSpec(memory_space=pltpu.VMEM),
        scratch_shapes=[
            pltpu.VMEM((rows, block), f32),
            pltpu.VMEM((2 * steps, rows, block), f32),
            pltpu.VMEM((block, depth_d), bf16),
            pltpu.VMEM((block, depth_c), bf16),
            pltpu.VMEM((2, depth_d, piece), bf16),
            pltpu.VMEM((2, depth_c, piece), bf16),
            pltpu.VMEM((block, 3 * dims + 16), f32),
            pltpu.SemaphoreType.DMA((2 * steps, parts)),
            pltpu.SemaphoreType.DMA((2 * steps, parts)),
        ],
        compiler_params=pltpu.CompilerParams(collective_id=0, has_side_effects=True),
    )(coords, alpha, probe_solves, probes, lengthscale)


def solution(mesh):
    return jax.shard_map(
        on_device,
        mesh=mesh,
        in_specs=(
            P(None, ("groups", "blk")),
            P(("groups", "blk")),
            P(None, ("groups", "blk")),
            P(None, ("groups", "blk")),
            P(),
        ),
        out_specs=P(None, ("groups", "blk")),
        check_vma=False,
    )
```
